256 devices in a mesh: grow: 16 (over y_lo, x, core), gcol: 16 (over z, y_hi).
Axes of the slice: x: 4, y: 4 (y_hi: 2, y_lo: 2; y = y_hi * 2 + y_lo), z: 8, core: 2. Of those that a mesh axis runs over, the one named last changes fastest.
Arguments:
- eps_static: float32 [12288, 12288], P('grow', 'gcol'), may hold values from -1.8 to 1.8
- eps_imag: float32 [12288, 12288], P('grow', 'gcol'), may hold values from -1.8 to 1.8
- frequency_grid: float32 [3], replicated, may hold values from 0.1 to 2
- band_energy: float32 [32], replicated, may hold values from -2 to 2
- pair_elements: bfloat16 [32, 64, 12288], P('grow', None, 'gcol'), may hold values from -0.0546875 to 0.0546875
Outputs:
- sigma: float32 [3, 64], P(None, 'gcol')
The draws below stay inside these ranges and needn't reach their ends.
All inputs are finite; a program needn't handle non-finite values.
Results may differ from the reference program's by a relative error of at most 0.0019.
Values may be sent and summed in bfloat16 or wider, within the bound.
A program may use at most 64 MiB of HBM per device.

```python
import math
import jax
import jax.numpy as jnp
from jax import lax

NG = 12288
STATES = 64
BANDS = 32
NE = 3


def block_levels(key, extent, cuts, low, high):
    level, own = 1.0, jax.random.fold_in(key, 6)
    for position, parts in cuts:
        heights = jnp.exp(jax.random.uniform(jax.random.fold_in(own, position), (parts,), jnp.float32, low / len(cuts), high / len(cuts)))
        level = level * jnp.repeat(heights, extent[position] // parts).reshape([-1 if axis == position else 1 for axis in range(len(extent))])
    return level


def gaussian(own_key, dims, scale, limit, cuts=(), kind=jnp.bfloat16):
    entries = scale * jax.random.normal(own_key, dims, jnp.float32)
    if cuts:
        entries = entries * block_levels(own_key, dims, cuts, -0.22, 0.18)
    return jnp.clip(entries, -limit, limit).astype(kind)


def setup_inputs(seed: int = 0) -> dict:
    arg_keys = jax.random.split(jax.random.key(seed), 6)
    eps_static = gaussian(arg_keys[0], (NG, NG), 0.3, 1.8, ((0, 16), (1, 16)), jnp.float32)
    eps_imag = gaussian(arg_keys[1], (NG, NG), 0.3, 1.8, ((0, 16), (1, 16)), jnp.float32)
    frequency_grid = jnp.clip(jnp.exp(jax.random.uniform(arg_keys[2], (NE,), jnp.float32, math.log(0.1), math.log(2.0))), 0.1, 2.0)
    band_energy = jnp.clip(jax.random.uniform(arg_keys[3], (BANDS,), jnp.float32, -2.0, 2.0), -2.0, 2.0)
    pair_elements = gaussian(arg_keys[4], (BANDS, STATES, NG), NG ** -0.5, 0.0546875, ((0, 16), (2, 16)))
    return dict(eps_static=eps_static, eps_imag=eps_imag, frequency_grid=frequency_grid, band_energy=band_energy, pair_elements=pair_elements)


def pole_kernels(static_rows, imag_rows, kronecker, frequency_grid):
    static_part = static_rows - kronecker
    imag_part = imag_rows - kronecker
    spread = static_part - imag_part
    pole_square = (imag_part * imag_part + 0.25) / (spread * spread + 0.25)
    pole_freq = jnp.sqrt(pole_square)
    strength = -static_part * pole_square
    return [(strength / (pole_freq * (pole_freq + frequency_grid[point]))).astype(jnp.bfloat16) for point in range(NE)]

def reference(eps_static, eps_imag, frequency_grid, band_energy, pair_elements):
    blocks = 16
    height = NG // blocks
    rows_all = pair_elements.reshape(BANDS * STATES, NG).astype(jnp.float32)
    col_ids = lax.iota(jnp.int32, NG)
    row_ids = lax.iota(jnp.int32, height)

    def advance(block, quad):
        start = (block * height).astype(jnp.int32)
        static_rows = lax.dynamic_slice_in_dim(eps_static, start, height, 0)
        imag_rows = lax.dynamic_slice_in_dim(eps_imag, start, height, 0)
        kronecker = ((start + row_ids)[:, None] == col_ids[None, :]).astype(jnp.float32)
        kernels = pole_kernels(static_rows, imag_rows, kronecker, frequency_grid)
        left = lax.dynamic_slice_in_dim(rows_all, start, height, 1)
        terms = []
        for kernel in kernels:
            wide = lax.optimization_barrier(kernel).astype(jnp.float32)
            projected = jnp.dot(left, wide, precision=lax.Precision.HIGHEST)
            terms.append(lax.optimization_barrier(jnp.sum(projected * rows_all, axis=1)))
        return quad + jnp.stack(terms)
    quad = lax.fori_loop(0, blocks, advance, jnp.zeros((NE, BANDS * STATES), jnp.float32))
    quad = quad.reshape(NE, BANDS, STATES)
    offset = frequency_grid[:, None] - band_energy[None, :]
    weight = 1.0 / (1.0 + offset * offset)
    return jnp.einsum('em,ems->es', weight, quad)
```

```python
import jax
import jax.numpy as jnp
from jax import lax
from jax.experimental import pallas as pl
from jax.experimental.pallas import tpu as pltpu
from jax.sharding import Mesh
from jax.sharding import PartitionSpec as P

NE = 3
NX = 4
NZ = 8
GROW = ("grow_0", "grow_1", "grow_2")
GCOL = ("gcol_0", "gcol_1")
MESH = pl.DeviceIdType.MESH
PEERS = ((0, 1), (0, 3), (1, 0), (1, 1), (1, 3), (0, 2), (1, 2))
SLICE = 16


def kernel(
    static_hbm, imag_hbm, freq, band, pair_hbm, out,
    rowp, colp, kmat, stat, imag, acc, red1, red2,
    in_sem, row_recv, row_send, col_recv, col_send, r1_recv, r1_send, r2_recv, r2_send,
):
    ylo, x, core = (lax.axis_index(a) for a in GROW)
    z, yhi = (lax.axis_index(a) for a in GCOL)
    plane = 4 * ylo + x
    row = plane * 2 + core
    col = z * 2 + yhi
    own_source = jnp.logical_and(plane == z, core == yhi)

    loads = [
        pltpu.make_async_copy(pair_hbm, colp.at[row], in_sem.at[0]),
        pltpu.make_async_copy(static_hbm, stat, in_sem.at[1]),
        pltpu.make_async_copy(imag_hbm, imag, in_sem.at[2]),
    ]
    for load in loads:
        load.start()

    barrier = pltpu.get_barrier_semaphore()

    def greet(device):
        pl.semaphore_signal(barrier, inc=1, device_id=device, device_id_type=MESH)

    for k in range(2):
        @pl.when(jnp.logical_not(jnp.logical_and(plane == z, jnp.logical_and(core == yhi, core == k))))
        def _():
            greet((z // NX, z % NX, k, plane, core))

    @pl.loop(1, 16)
    def _(i):
        dz, dh = i // 2, i % 2
        greet((ylo, x, core, (z + dz) % NZ, (yhi + dh) % 2))
        greet(((ylo + i // 8) % 2, (x + (i // 2) % 4) % NX, (core + i % 2) % 2, z, yhi))

    loads[0].wait()
    pl.semaphore_wait(barrier, 32 - own_source.astype(jnp.int32))

    def scatter(h):
        return pltpu.make_async_remote_copy(
            src_ref=colp.at[row], dst_ref=rowp.at[row], send_sem=row_send.at[h], recv_sem=row_recv.at[row],
            device_id=(z // NX, z % NX, yhi, plane, h), device_id_type=MESH,
        )

    for h in range(2):
        mine = jnp.logical_and(own_source, yhi == h)

        @pl.when(jnp.logical_not(mine))
        def _():
            scatter(h).start()

        @pl.when(mine)
        def _():
            pltpu.make_async_copy(pair_hbm, rowp.at[row], row_recv.at[row]).start()

    def to_partner(slot, sem):
        return pltpu.make_async_remote_copy(
            src_ref=colp.at[slot], dst_ref=colp.at[slot], send_sem=col_send.at[sem], recv_sem=col_recv.at[slot],
            device_id=(ylo, x, 1 - core, z, yhi), device_id_type=MESH,
        )

    to_partner(row, 7).start()
    own_sends = []
    for i, (dy, dx) in enumerate(PEERS):
        send = pltpu.make_async_remote_copy(
            src_ref=colp.at[row], dst_ref=colp.at[row], send_sem=col_send.at[i], recv_sem=col_recv.at[row],
            device_id=((ylo + dy) % 2, (x + dx) % NX, core, z, yhi), device_id_type=MESH,
        )
        send.start()
        own_sends.append(send)

    loads[1].wait()
    loads[2].wait()
    diagonal = row * stat.shape[0] - col * stat.shape[1]
    acc[...] = jnp.zeros_like(acc)

    @pl.loop(0, stat.shape[0] // SLICE)
    def _(i):
        start = pl.multiple_of(i * SLICE, SLICE)
        rows = pl.ds(start, SLICE)
        shape = (SLICE, stat.shape[1])
        ahead = lax.broadcasted_iota(jnp.int32, shape, 1) - lax.broadcasted_iota(jnp.int32, shape, 0)
        one = jnp.where(ahead == diagonal + start, 1.0, 0.0).astype(jnp.float32)
        s = stat[rows, :] - one
        g = imag[rows, :] - one
        d = s - g
        pole = jnp.sqrt((g * g + 0.25) / (d * d + 0.25))
        top = -s * pole
        for e in range(NE):
            kmat[e, rows, :] = (top / (pole + freq[e])).astype(jnp.bfloat16)

    def row_slot(slot):
        return pltpu.make_async_copy(rowp.at[slot], rowp.at[slot], row_recv.at[slot])

    def col_slot(slot):
        return pltpu.make_async_copy(colp.at[slot], colp.at[slot], col_recv.at[slot])

    def ring(slot, sem, step):
        return pltpu.make_async_remote_copy(
            src_ref=rowp.at[slot], dst_ref=rowp.at[slot], send_sem=row_send.at[sem], recv_sem=row_recv.at[slot],
            device_id=(ylo, x, core, (z + NZ + step) % NZ, yhi), device_id_type=MESH,
        )

    def up_slot(i):
        return 2 * ((z + NZ - i // 2) % NZ) + i % 2

    def down_slot(i):
        return 2 * ((z + i // 2) % NZ) + 1 - i % 2

    def piece_of(j):
        return (z + NZ + ((j + 1) // 2) * (2 * (j % 2) - 1)) % NZ

    def compute(piece):
        left = rowp[pl.ds(2 * piece, 2)].reshape(256, rowp.shape[2])

        @pl.loop(0, NE)
        def _(e):
            projected = jnp.dot(left, kmat[e], preferred_element_type=jnp.float32)
            terms = projected * colp[pl.ds(2 * piece, 2)].reshape(256, colp.shape[2]).astype(jnp.float32)
            lanes = terms[:, 0:128]
            for g in range(1, 6):
                lanes = lanes + terms[:, g * 128:(g + 1) * 128]
            total = acc[e, 0:64, :]
            for b in range(4):
                offset = freq[e] - band[4 * piece + b]
                weight = 1.0 / (1.0 + jnp.full((1, 128), offset * offset, jnp.float32))
                total = total + weight * lanes[b * 64:(b + 1) * 64, :]
            acc[e, 0:64, :] = total

    for i in range(7):
        if i != 1:
            row_slot(up_slot(i)).wait()
            row_slot(down_slot(i)).wait()
        ring(up_slot(i), 2 + 2 * i, 1).start()
        ring(down_slot(i), 3 + 2 * i, -1).start()
        for p in (2 * i, 2 * i + 1):
            if p < len(PEERS):
                dy, dx = PEERS[p]
                slot = 2 * (4 * ((ylo + NZ - dy) % 2) + (x + NX - dx) % NX) + core
                col_slot(slot).wait()
                to_partner(slot, 8 + p).start()
        if i == 4:
            for q in range(8):
                col_slot(2 * q + 1 - core).wait()

            @pl.loop(0, 3)
            def _(j):
                compute(piece_of(j))
        if i == 6:
            @pl.loop(3, 5)
            def _(j):
                compute(piece_of(j))

    row_slot(up_slot(7)).wait()
    row_slot(down_slot(7)).wait()

    @pl.loop(5, 7)
    def _(j):
        compute(piece_of(j))

    far = (z + 4) % NZ
    row_slot(2 * far).wait()
    row_slot(2 * far + 1).wait()
    compute(far)

    ones = jnp.ones((8, 128), jnp.float32)
    which = lax.broadcasted_iota(jnp.int32, (8, 128), 0)
    tile = jnp.zeros((8, 128), jnp.float32)
    for e in range(NE):
        summed = lax.dot_general(
            ones, acc[e], (((1,), (1,)), ((), ())),
            precision=lax.Precision.HIGHEST, preferred_element_type=jnp.float32,
        )
        tile = tile + jnp.where(which == e, summed, 0.0)

    def exchange(buffer, me, value, target, recv, send):
        buffer[me] = value

        def copy(i, device):
            return pltpu.make_async_remote_copy(
                src_ref=buffer.at[me], dst_ref=buffer.at[me], send_sem=send.at[i], recv_sem=recv.at[me],
                device_id=device, device_id_type=MESH,
            )

        @pl.loop(1, 16)
        def _(i):
            copy(i, target(i)).start()

        @pl.loop(1, 16)
        def _(i):
            slot = (me + i) % 16
            pltpu.make_async_copy(buffer.at[slot], buffer.at[slot], recv.at[slot]).wait()

        @pl.loop(1, 16)
        def _(i):
            copy(i, target(i)).wait_send()

        total = buffer[0]
        for i in range(1, 16):
            total = total + buffer[i]
        return total

    tile = exchange(red1, col, tile, lambda i: (ylo, x, core, (z + i // 2) % NZ, (yhi + i % 2) % 2), r1_recv, r1_send)
    out[...] = exchange(
        red2, row, tile,
        lambda i: ((ylo + i // 8) % 2, (x + (i // 2) % 4) % NX, (core + i % 2) % 2, z, yhi), r2_recv, r2_send,
    )

    for h in range(2):
        @pl.when(jnp.logical_not(jnp.logical_and(own_source, yhi == h)))
        def _():
            scatter(h).wait_send()
    for send in own_sends:
        send.wait_send()
    to_partner(row, 7).wait_send()
    for p, (dy, dx) in enumerate(PEERS):
        slot = 2 * (4 * ((ylo + NZ - dy) % 2) + (x + NX - dx) % NX) + core
        to_partner(slot, 8 + p).wait_send()
    for i in range(7):
        ring(up_slot(i), 2 + 2 * i, 1).wait_send()
        ring(down_slot(i), 3 + 2 * i, -1).wait_send()


def shards(eps_static, eps_imag, frequency_grid, band_energy, pair_elements):
    height, breadth = eps_static.shape
    rows = pair_elements.shape[0] * pair_elements.shape[1]
    pair = pair_elements.reshape(rows, breadth)
    anywhere = pl.BlockSpec(memory_space=pl.ANY)
    scalars = pl.BlockSpec(memory_space=pltpu.SMEM)
    dma = pltpu.SemaphoreType.DMA
    summed = pl.pallas_call(
        kernel,
        out_shape=jax.ShapeDtypeStruct((8, 128), jnp.float32),
        in_specs=[anywhere, anywhere, scalars, scalars, anywhere],
        out_specs=pl.BlockSpec(memory_space=pltpu.VMEM),
        scratch_shapes=[
            pltpu.VMEM((16, rows, height), jnp.bfloat16),
            pltpu.VMEM((16, rows, breadth), jnp.bfloat16),
            pltpu.VMEM((NE, height, breadth), jnp.bfloat16),
            pltpu.VMEM((height, breadth), jnp.float32),
            pltpu.VMEM((height, breadth), jnp.float32),
            pltpu.VMEM((NE, 128, 128), jnp.float32),
            pltpu.VMEM((16, 8, 128), jnp.float32),
            pltpu.VMEM((16, 8, 128), jnp.float32),
            dma((3,)), dma((16,)), dma((16,)), dma((16,)), dma((15,)),
            dma((16,)), dma((16,)), dma((16,)), dma((16,)),
        ],
        compiler_params=pltpu.CompilerParams(
            collective_id=0, has_side_effects=True, vmem_limit_bytes=60 * 1024 * 1024
        ),
    )(eps_static, eps_imag, frequency_grid, band_energy, pair)
    states = pair_elements.shape[1] // lax.axis_size(GCOL)
    return lax.dynamic_slice(summed, (0, lax.axis_index(GCOL) * states), (NE, states))


def solution(mesh):
    finer = Mesh(
        mesh.devices.reshape(2, 4, 2, 8, 2), ("grow_0", "grow_1", "grow_2", "gcol_0", "gcol_1")
    )
    in_specs = (P(GROW, GCOL), P(GROW, GCOL), P(), P(), P(GROW, None, GCOL))
    out_specs = P(None, GCOL)
    return jax.shard_map(
        shards, mesh=finer, in_specs=in_specs, out_specs=out_specs, check_vma=False
    )
```

```python
import jax
import jax.numpy as jnp
from jax import lax
from jax.experimental import pallas as pl
from jax.experimental.pallas import tpu as pltpu
from jax.sharding import Mesh
from jax.sharding import PartitionSpec as P

NE = 3
NX = 4
NZ = 8
GROW = ("grow_0", "grow_1", "grow_2")
GCOL = ("gcol_0", "gcol_1")
MESH = pl.DeviceIdType.MESH
SLICE = 16
ACROSS = (0, 2, -2, 4)
EVERY = (0, 1, -1, 2, -2, 3, -3, 4)


def kernel(
    static_hbm, imag_hbm, freq, band, pair_hbm, out,
    rowp, colp, kmat, stat, imag, acc, red1, red2,
    in_sem, sent, row_recv, col_recv, r1_recv, r1_send, r2_recv, r2_send,
):
    ylo, x, core = (lax.axis_index(a) for a in GROW)
    z, yhi = (lax.axis_index(a) for a in GCOL)
    plane = NX * ylo + x
    row = plane * 2 + core
    col = z * 2 + yhi
    half = rowp.shape[1] // 2
    partner = (ylo, x, 1 - core, z, yhi)

    def in_plane(i):
        return ((ylo + (i // 4) % 2) % 2, (x + i % 4) % NX, core, z, (yhi + i // 8) % 2)

    def along_z(i):
        return (ylo, x, (core + i % 2) % 2, (z + i // 2) % NZ, yhi)

    loads = [
        pltpu.make_async_copy(pair_hbm, colp.at[row], in_sem.at[0]),
        pltpu.make_async_copy(static_hbm, stat, in_sem.at[1]),
        pltpu.make_async_copy(imag_hbm, imag, in_sem.at[2]),
    ]
    for load in loads:
        load.start()

    barrier = pltpu.get_barrier_semaphore()

    def greet(device):
        pl.semaphore_signal(barrier, inc=1, device_id=device, device_id_type=MESH)

    stays = jnp.logical_and(jnp.logical_and(plane == z, z == 0), core == yhi)
    origin = (z + plane) % NZ

    @pl.when(jnp.logical_not(stays))
    def _():
        greet((origin // NX, origin % NX, yhi, plane, core))

    @pl.loop(1, 16)
    def _(i):
        greet(in_plane(i))
        greet(along_z(i))

    loads[1].wait()
    loads[2].wait()
    diagonal = row * stat.shape[0] - col * stat.shape[1]
    acc[...] = jnp.zeros_like(acc)

    @pl.loop(0, stat.shape[0] // SLICE)
    def _(i):
        start = pl.multiple_of(i * SLICE, SLICE)
        rows = pl.ds(start, SLICE)
        shape = (SLICE, stat.shape[1])
        ahead = lax.broadcasted_iota(jnp.int32, shape, 1) - lax.broadcasted_iota(jnp.int32, shape, 0)
        one = jnp.where(ahead == diagonal + start, 1.0, 0.0).astype(jnp.float32)
        s = stat[rows, :] - one
        g = imag[rows, :] - one
        d = s - g
        pole = jnp.sqrt((g * g + 0.25) / (d * d + 0.25))
        top = -s * pole
        for e in range(NE):
            kmat[e, rows, :] = (top / (pole + freq[e])).astype(jnp.bfloat16)

    loads[0].wait()
    pl.semaphore_wait(barrier, 31 - stays.astype(jnp.int32))

    started = []

    def send(src, dst, recv, device):
        copy = pltpu.make_async_remote_copy(
            src_ref=src, dst_ref=dst, send_sem=sent.at[len(started)], recv_sem=recv,
            device_id=device, device_id_type=MESH,
        )
        started.append(copy)
        return copy

    first = send(colp.at[row], rowp.at[row], row_recv.at[2 * row], (z // NX, z % NX, yhi, (plane + NZ - z) % NZ, core))

    @pl.when(jnp.logical_not(stays))
    def _():
        first.start()

    @pl.when(stays)
    def _():
        pltpu.make_async_copy(pair_hbm, rowp.at[row], row_recv.at[2 * row]).start()

    def block(chain, far):
        return 2 * ((z + plane + 2 * NZ - far) % NZ) + (yhi + chain) % 2

    arrived = set()

    def need(chain, far, part):
        whole = far == 0 or (chain == 1 and far in ACROSS)
        key = (chain, far) if whole else (chain, far, part)
        if key in arrived:
            return
        arrived.add(key)
        b = block(chain, far)
        if whole:
            ref, sem = rowp.at[b], row_recv.at[2 * b]
        else:
            ref, sem = rowp.at[b, pl.ds(part * half, half)], row_recv.at[2 * b + part]
        pltpu.make_async_copy(ref, ref, sem).wait()

    def along(chain, far, parts=((0, 1), (0, 1))):
        for step, side in ((1, parts[0]), (-1, parts[1])):
            for part in side:
                need(chain, step * far, part)
                b = block(chain, step * far)
                ref = rowp.at[b, pl.ds(part * half, half)]
                send(ref, ref, row_recv.at[2 * b + part], (ylo, x, core, (z + NZ + step) % NZ, yhi)).start()

    def across(far):
        need(0, far, 0)
        need(0, far, 1)
        b = block(0, far)
        send(rowp.at[b], rowp.at[b], row_recv.at[2 * b], (ylo, x, core, z, 1 - yhi)).start()

    def col_slot(a, b, c):
        return 2 * (NX * a + b) + c

    def col_wait(slot):
        pltpu.make_async_copy(colp.at[slot], colp.at[slot], col_recv.at[slot]).wait()

    def col_send(slot, device):
        send(colp.at[slot], colp.at[slot], col_recv.at[slot], device).start()

    def relay(i):
        slot = col_slot((ylo + i // 3) % 2, (x + NX - (1, 3, 2)[i % 3]) % NX, core)
        col_wait(slot)
        col_send(slot, partner)

    def compute(b0, b1):
        left = jnp.concatenate([rowp[b0], rowp[b1]], axis=0)
        rows = rowp.shape[1]

        @pl.loop(0, NE)
        def _(e):
            projected = jnp.dot(left, kmat[e], preferred_element_type=jnp.float32)
            total = acc[e, 0:half, :]
            for n, b in enumerate((b0, b1)):
                terms = projected[n * rows:(n + 1) * rows] * colp[b].astype(jnp.float32)
                lanes = terms[:, 0:128]
                for g in range(1, terms.shape[1] // 128):
                    lanes = lanes + terms[:, g * 128:(g + 1) * 128]
                for part in range(2):
                    offset = freq[e] - band[2 * b + part]
                    weight = 1.0 / (1.0 + jnp.full((1, 128), offset * offset, jnp.float32))
                    total = total + weight * lanes[part * half:(part + 1) * half, :]
            acc[e, 0:half, :] = total

    def compute_pair(chain, far):
        for f in (far, -far):
            need(chain, f, 0)
            need(chain, f, 1)
        compute(block(chain, far), block(chain, -far))

    def compute_both(far):
        for chain in range(2):
            need(chain, far, 0)
            need(chain, far, 1)
        compute(block(0, far), block(1, far))

    col_send(row, (1 - ylo, x, core, z, yhi))
    col_send(row, partner)
    for dx in (1, 3, 2):
        col_send(row, (ylo, (x + dx) % NX, core, z, yhi))

    along(0, 0)
    across(0)
    along(0, 1)
    neighbour = col_slot(1 - ylo, x, core)
    col_wait(neighbour)
    for dx in (1, 3, 2):
        col_send(neighbour, (ylo, (x + dx) % NX, core, z, yhi))
    col_send(neighbour, partner)
    relay(0)
    along(0, 2)
    relay(1)
    across(2)
    across(-2)
    along(0, 3, ((0,), (1,)))
    along(1, 0)
    for i in range(2, 6):
        relay(i)
    for a in range(2):
        for b in range(NX):
            col_wait(col_slot(a, b, 1 - core))
    compute_both(0)
    across(4)
    compute_pair(0, 1)
    compute_pair(0, 2)
    along(1, 2)
    compute_pair(0, 3)
    compute_pair(1, 2)
    compute_pair(1, 1)
    compute_both(4)
    compute_pair(1, 3)

    ones = jnp.ones((8, 128), jnp.float32)
    which = lax.broadcasted_iota(jnp.int32, (8, 128), 0)
    tile = jnp.zeros((8, 128), jnp.float32)
    for e in range(NE):
        summed = lax.dot_general(
            ones, acc[e], (((1,), (1,)), ((), ())),
            precision=lax.Precision.HIGHEST, preferred_element_type=jnp.float32,
        )
        tile = tile + jnp.where(which == e, summed, 0.0)

    def exchange(buffer, me, value, target, recv, sem):
        buffer[me] = value

        def copy(i):
            return pltpu.make_async_remote_copy(
                src_ref=buffer.at[me], dst_ref=buffer.at[me], send_sem=sem.at[i], recv_sem=recv.at[me],
                device_id=target(i), device_id_type=MESH,
            )

        @pl.loop(1, 16)
        def _(i):
            copy(i).start()

        @pl.loop(1, 16)
        def _(i):
            slot = (me + i) % 16
            pltpu.make_async_copy(buffer.at[slot], buffer.at[slot], recv.at[slot]).wait()

        @pl.loop(1, 16)
        def _(i):
            copy(i).wait_send()

        total = buffer[0]
        for i in range(1, 16):
            total = total + buffer[i]
        return total

    tile = exchange(red1, NX * (2 * yhi + ylo) + x, tile, in_plane, r1_recv, r1_send)
    out[...] = exchange(red2, 2 * z + core, tile, along_z, r2_recv, r2_send)

    @pl.when(jnp.logical_not(stays))
    def _():
        first.wait_send()

    for copy in started[1:]:
        copy.wait_send()


def shards(eps_static, eps_imag, frequency_grid, band_energy, pair_elements):
    height, breadth = eps_static.shape
    rows = pair_elements.shape[0] * pair_elements.shape[1]
    pair = pair_elements.reshape(rows, breadth)
    anywhere = pl.BlockSpec(memory_space=pl.ANY)
    scalars = pl.BlockSpec(memory_space=pltpu.SMEM)
    dma = pltpu.SemaphoreType.DMA
    summed = pl.pallas_call(
        kernel,
        out_shape=jax.ShapeDtypeStruct((8, 128), jnp.float32),
        in_specs=[anywhere, anywhere, scalars, scalars, anywhere],
        out_specs=pl.BlockSpec(memory_space=pltpu.VMEM),
        scratch_shapes=[
            pltpu.VMEM((16, rows, height), jnp.bfloat16),
            pltpu.VMEM((16, rows, breadth), jnp.bfloat16),
            pltpu.VMEM((NE, height, breadth), jnp.bfloat16),
            pltpu.VMEM((height, breadth), jnp.float32),
            pltpu.VMEM((height, breadth), jnp.float32),
            pltpu.VMEM((NE, 128, 128), jnp.float32),
            pltpu.VMEM((16, 8, 128), jnp.float32),
            pltpu.VMEM((16, 8, 128), jnp.float32),
            dma((3,)), dma((48,)), dma((32,)), dma((16,)),
            dma((16,)), dma((16,)), dma((16,)), dma((16,)),
        ],
        compiler_params=pltpu.CompilerParams(
            collective_id=0, has_side_effects=True, vmem_limit_bytes=60 * 1024 * 1024
        ),
    )(eps_static, eps_imag, frequency_grid, band_energy, pair)
    states = pair_elements.shape[1] // lax.axis_size(GCOL)
    return lax.dynamic_slice(summed, (0, lax.axis_index(GCOL) * states), (NE, states))


def solution(mesh):
    finer = Mesh(
        mesh.devices.reshape(2, 4, 2, 8, 2), ("grow_0", "grow_1", "grow_2", "gcol_0", "gcol_1")
    )
    in_specs = (P(GROW, GCOL), P(GROW, GCOL), P(), P(), P(GROW, None, GCOL))
    out_specs = P(None, GCOL)
    return jax.shard_map(
        shards, mesh=finer, in_specs=in_specs, out_specs=out_specs, check_vma=False
    )
```

```python
import jax
import jax.numpy as jnp
from jax import lax
from jax.experimental import pallas as pl
from jax.experimental.pallas import tpu as pltpu
from jax.sharding import Mesh
from jax.sharding import PartitionSpec as P

NE = 3
NX = 4
NZ = 8
GROW = ("grow_0", "grow_1", "grow_2")
GCOL = ("gcol_0", "gcol_1")
MESH = pl.DeviceIdType.MESH
SLICE = 16
EVERY = (0, 1, -1, 2, -2, 3, -3, 4)
PROGRAM = (
    ("n",),
    ("z", 0, 0, 0), ("y", 0, 0),
    ("r", 0), ("r", 1),
    ("z", 0, 0, 1), ("y", 0, 1), ("z", 0, 1, 0), ("y", 1, 0),
    ("r", 2),
    ("y", -1, 0), ("z", 0, 1, 1), ("y", 1, 1),
    ("d", (0, 0), (1, 0)),
    ("z", 0, 2, 0),
    ("r", 3),
    ("y", -1, 1), ("z", 0, 2, 1),
    ("d", (0, 1), (0, -1)),
    ("z", 1, 1, 0), ("r", 4), ("y", 3, 1), ("z", 0, 3, 0), ("z", 0, 3, 1),
    ("d", (0, 2), (0, -2)),
    ("y", -3, 1), ("z", 1, 1, 1),
    ("r", 5), ("y", 4, 0), ("z", 1, 2, 0),
    ("w",),
    ("c", (1, 1), (1, -1)),
    ("z", 1, 3, 1),
    ("c", (0, 3), (0, -3)),
    ("m", (0, 0), (1, 0), (0, 1), (0, -1), (0, 2), (0, -2)),
    ("c", (0, 4),), ("c", (1, 2), (1, -2)), ("c", (1, 3), (1, -3)), ("c", (1, 4),),
)


def kernel(
    static_hbm, imag_hbm, freq, band, pair_hbm, out,
    rowp, colp, kmat, stat, imag, ahead, acc, red1, red2,
    in_sem, sent, row_recv, col_recv, r1_recv, r1_send, r2_recv, r2_send,
):
    ylo, x, core = (lax.axis_index(a) for a in GROW)
    z, yhi = (lax.axis_index(a) for a in GCOL)
    plane = NX * ylo + x
    row = plane * 2 + core
    col = z * 2 + yhi
    half = rowp.shape[1] // 2
    partner = (ylo, x, 1 - core, z, yhi)
    xs = [lax.rem(x + i, NX) for i in range(NX)]
    zs = [lax.rem(z + i, NZ) for i in range(NZ)]
    cores, ylos, yhis = (core, 1 - core), (ylo, 1 - ylo), (yhi, 1 - yhi)
    in_plane = [
        (ylos[a], xs[b], core, z, yhis[c]) for c in (1, 0) for b in (2, 1, 3, 0) for a in (1, 0) if (a, b, c) != (0, 0, 0)
    ]
    along_z = [
        (ylo, x, cores[a], zs[b], yhi) for b in (4, 3, 5, 2, 6, 1, 7, 0) for a in (1, 0) if (a, b) != (0, 0)
    ]

    loads = [
        pltpu.make_async_copy(pair_hbm, colp.at[row], in_sem.at[0]),
        pltpu.make_async_copy(static_hbm, stat, in_sem.at[1]),
        pltpu.make_async_copy(imag_hbm, imag, in_sem.at[2]),
    ]
    for load in loads:
        load.start()

    barrier = pltpu.get_barrier_semaphore()

    def greet(device):
        pl.semaphore_signal(barrier, inc=1, device_id=device, device_id_type=MESH)

    stays = jnp.logical_and(jnp.logical_and(plane == z, z == 0), core == yhi)
    origin = lax.rem(z + plane, NZ)

    @pl.when(jnp.logical_not(stays))
    def _():
        greet((origin // NX, lax.rem(origin, NX), yhi, plane, core))

    for device in along_z + in_plane:
        greet(device)

    loads[0].wait()
    pl.semaphore_wait(barrier, 31 - stays.astype(jnp.int32))

    started = []

    def send(src, dst, recv, device):
        copy = pltpu.make_async_remote_copy(
            src_ref=src, dst_ref=dst, send_sem=sent.at[len(started)], recv_sem=recv,
            device_id=device, device_id_type=MESH,
        )
        started.append(copy)
        return copy

    place = (z // NX, lax.rem(z, NX), yhi, lax.rem(plane + NZ - z, NZ), core)

    def piece(panel, slot, part):
        return panel.at[slot, pl.ds(part * half, half)]

    first = [send(piece(colp, row, t), piece(rowp, row, t), row_recv.at[2 * row + t], place) for t in range(2)]

    @pl.when(jnp.logical_not(stays))
    def _():
        for copy in first:
            copy.start()

    @pl.when(stays)
    def _():
        for t in range(2):
            pltpu.make_async_copy(pair_hbm.at[pl.ds(t * half, half)], piece(rowp, row, t), row_recv.at[2 * row + t]).start()

    pieces = {far: 2 * lax.rem(z + plane + 2 * NZ - far, NZ) for far in EVERY}
    pieces[-4] = pieces[4]

    def block(chain, far):
        return pieces[far] + yhis[chain]

    arrived = set()

    def need(chain, far, part):
        far = 4 if far == -4 else far
        if (chain, far, part) not in arrived:
            arrived.add((chain, far, part))
            b = block(chain, far)
            pltpu.make_async_copy(piece(rowp, b, part), piece(rowp, b, part), row_recv.at[2 * b + part]).wait()

    def pass_on(chain, far, part, device):
        need(chain, far, part)
        b = block(chain, far)
        send(piece(rowp, b, part), piece(rowp, b, part), row_recv.at[2 * b + part], device).start()

    def along(chain, far, part):
        for way in (1, -1) if far < 3 else ((1,) if part == 0 else (-1,)):
            pass_on(chain, way * far, part, (ylo, x, core, zs[way % NZ], yhi))

    def across(far, part):
        pass_on(0, far, part, (ylo, x, core, z, yhis[1]))

    def col_slot(a, b, c):
        return 2 * (NX * a + b) + c

    def col_wait(slot):
        pltpu.make_async_copy(colp.at[slot], colp.at[slot], col_recv.at[slot]).wait()

    def col_send(slot, device):
        send(colp.at[slot], colp.at[slot], col_recv.at[slot], device).start()

    def relay(i):
        slot = col_slot(ylos[i // 3], xs[(3, 1, 2)[i % 3]], core)
        col_wait(slot)
        col_send(slot, partner)

    def project(blocks, e):
        left = jnp.concatenate([rowp[b] for b in blocks], axis=0)
        return jnp.dot(left, kmat[e], preferred_element_type=jnp.float32)

    def weighted(projected, b, e):
        terms = projected * colp[b].astype(jnp.float32)
        lanes = terms[:, 0:128]
        for g in range(1, terms.shape[1] // 128):
            lanes = lanes + terms[:, g * 128:(g + 1) * 128]
        total = 0.0
        for part in range(2):
            offset = freq[e] - band[2 * b + part]
            weight = 1.0 / (1.0 + jnp.full((1, 128), offset * offset, jnp.float32))
            total = total + weight * lanes[part * half:(part + 1) * half, :]
        return total

    kept = {}

    def rows_of(n):
        return slice(n * rowp.shape[1], (n + 1) * rowp.shape[1])

    def project_ahead(keys):
        blocks = [block(*key) for key in keys]
        for e in range(NE):
            projected = project(blocks, e)
            for n, key in enumerate(keys):
                ahead[kept.setdefault(key, len(kept)), e] = projected[rows_of(n)]

    def finish(keys):
        for e in range(NE):
            total = acc[e, 0:half, :]
            for key in keys:
                total = total + weighted(ahead[kept[key], e], block(*key), e)
            acc[e, 0:half, :] = total

    def compute(keys):
        blocks = [block(*key) for key in keys]
        for e in range(NE):
            projected = project(blocks, e)
            total = acc[e, 0:half, :]
            for n, b in enumerate(blocks):
                total = total + weighted(projected[rows_of(n)], b, e)
            acc[e, 0:half, :] = total

    col_send(row, (ylos[1], x, core, z, yhi))
    col_send(row, partner)
    for dx in (1, 3, 2):
        col_send(row, (ylo, xs[dx], core, z, yhi))

    loads[1].wait()
    loads[2].wait()
    diagonal = row * stat.shape[0] - col * stat.shape[1]
    acc[...] = jnp.zeros_like(acc)

    @pl.loop(0, stat.shape[0] // SLICE)
    def _(i):
        start = pl.multiple_of(i * SLICE, SLICE)
        rows = pl.ds(start, SLICE)
        shape = (SLICE, stat.shape[1])
        ahead = lax.broadcasted_iota(jnp.int32, shape, 1) - lax.broadcasted_iota(jnp.int32, shape, 0)
        one = jnp.where(ahead == diagonal + start, 1.0, 0.0).astype(jnp.float32)
        s = stat[rows, :] - one
        g = imag[rows, :] - one
        d = s - g
        pole = jnp.sqrt((g * g + 0.25) / (d * d + 0.25))
        top = -s * pole
        for e in range(NE):
            kmat[e, rows, :] = (top / (pole + freq[e])).astype(jnp.bfloat16)

    for op, *args in PROGRAM:
        if op == "z":
            along(*args)
        elif op == "y":
            across(*args)
        elif op == "n":
            neighbour = col_slot(ylos[1], x, core)
            col_wait(neighbour)
            for dx in (1, 3, 2):
                col_send(neighbour, (ylo, xs[dx], core, z, yhi))
            col_send(neighbour, partner)
        elif op == "r":
            relay(*args)
        elif op == "w":
            for a in range(2):
                for b in range(NX):
                    col_wait(col_slot(a, b, 1 - core))
        else:
            for chain, far in args:
                need(chain, far, 0)
                need(chain, far, 1)
            {"d": project_ahead, "m": finish, "c": compute}[op](args)

    ones = jnp.ones((8, 128), jnp.float32)
    which = lax.broadcasted_iota(jnp.int32, (8, 128), 0)
    tile = jnp.zeros((8, 128), jnp.float32)
    for e in range(NE):
        summed = lax.dot_general(
            ones, acc[e], (((1,), (1,)), ((), ())),
            precision=lax.Precision.HIGHEST, preferred_element_type=jnp.float32,
        )
        tile = tile + jnp.where(which == e, summed, 0.0)

    def exchange(buffer, me, value, devices, recv, sem):
        buffer[me] = value
        copies = [
            pltpu.make_async_remote_copy(
                src_ref=buffer.at[me], dst_ref=buffer.at[me], send_sem=sem.at[i], recv_sem=recv.at[me],
                device_id=device, device_id_type=MESH,
            )
            for i, device in enumerate(devices)
        ]
        for copy in copies:
            copy.start()
        for i in range(1, 16):
            slot = lax.rem(me + i, 16)
            pltpu.make_async_copy(buffer.at[slot], buffer.at[slot], recv.at[slot]).wait()
        total = buffer[0]
        for i in range(1, 16):
            total = total + buffer[i]
        return total, copies

    tile, last = exchange(red1, NX * (2 * yhi + ylo) + x, tile, in_plane, r1_recv, r1_send)
    out[...], more = exchange(red2, 2 * z + core, tile, along_z, r2_recv, r2_send)

    @pl.when(jnp.logical_not(stays))
    def _():
        for copy in first:
            copy.wait_send()

    for copy in started[2:] + last + more:
        copy.wait_send()


def shards(eps_static, eps_imag, frequency_grid, band_energy, pair_elements):
    height, breadth = eps_static.shape
    rows = pair_elements.shape[0] * pair_elements.shape[1]
    pair = pair_elements.reshape(rows, breadth)
    anywhere = pl.BlockSpec(memory_space=pl.ANY)
    scalars = pl.BlockSpec(memory_space=pltpu.SMEM)
    dma = pltpu.SemaphoreType.DMA
    summed = pl.pallas_call(
        kernel,
        out_shape=jax.ShapeDtypeStruct((8, 128), jnp.float32),
        in_specs=[anywhere, anywhere, scalars, scalars, anywhere],
        out_specs=pl.BlockSpec(memory_space=pltpu.VMEM),
        scratch_shapes=[
            pltpu.VMEM((16, rows, height), jnp.bfloat16),
            pltpu.VMEM((16, rows, breadth), jnp.bfloat16),
            pltpu.VMEM((NE, height, breadth), jnp.bfloat16),
            pltpu.VMEM((height, breadth), jnp.float32),
            pltpu.VMEM((height, breadth), jnp.float32),
            pltpu.VMEM((6, NE, rows, breadth), jnp.float32),
            pltpu.VMEM((NE, 128, 128), jnp.float32),
            pltpu.VMEM((16, 8, 128), jnp.float32),
            pltpu.VMEM((16, 8, 128), jnp.float32),
            dma((3,)), dma((80,)), dma((32,)), dma((16,)),
            dma((16,)), dma((16,)), dma((16,)), dma((16,)),
        ],
        compiler_params=pltpu.CompilerParams(
            collective_id=0, has_side_effects=True, vmem_limit_bytes=60 * 1024 * 1024
        ),
    )(eps_static, eps_imag, frequency_grid, band_energy, pair)
    states = pair_elements.shape[1] // lax.axis_size(GCOL)
    return lax.dynamic_slice(summed, (0, lax.axis_index(GCOL) * states), (NE, states))


def solution(mesh):
    finer = Mesh(
        mesh.devices.reshape(2, 4, 2, 8, 2), ("grow_0", "grow_1", "grow_2", "gcol_0", "gcol_1")
    )
    in_specs = (P(GROW, GCOL), P(GROW, GCOL), P(), P(), P(GROW, None, GCOL))
    out_specs = P(None, GCOL)
    return jax.shard_map(
        shards, mesh=finer, in_specs=in_specs, out_specs=out_specs, check_vma=False
    )
```

```python
import jax
import jax.numpy as jnp
from jax import lax
from jax.experimental import pallas as pl
from jax.experimental.pallas import tpu as pltpu
from jax.sharding import Mesh
from jax.sharding import PartitionSpec as P

NE = 3
NX = 4
NZ = 8
GROW = ("grow_0", "grow_1", "grow_2")
GCOL = ("gcol_0", "gcol_1")
MESH = pl.DeviceIdType.MESH
SLICE = 16
EVERY = (0, 1, -1, 2, -2, 3, -3, 4)
PROGRAM = (
    ("n",),
    ("z", 0, 0, 0), ("y", 0, 0),
    ("r", 0), ("r", 1),
    ("z", 0, 0, 1), ("y", 0, 1), ("z", 0, 1, 0), ("y", 1, 0),
    ("r", 2),
    ("y", -1, 0), ("z", 0, 1, 1), ("y", 1, 1),
    ("d", (0, 0), (1, 0)),
    ("z", 0, 2, 0),
    ("r", 3),
    ("y", -1, 1), ("z", 0, 2, 1),
    ("d", (0, 1), (0, -1)),
    ("z", 1, 1, 0), ("r", 4), ("y", 3, 1), ("z", 0, 3, 0), ("z", 0, 3, 1),
    ("d", (0, 2), (0, -2)),
    ("y", -3, 1), ("z", 1, 1, 1),
    ("r", 5), ("y", 4, 0), ("z", 1, 2, 0),
    ("w",),
    ("c", (1, 1), (1, -1)),
    ("z", 1, 3, 1),
    ("c", (0, 3), (0, -3)),
    ("m", (0, 0), (1, 0), (0, 1), (0, -1), (0, 2), (0, -2)),
    ("c", (0, 4),), ("c", (1, 2), (1, -2)), ("c", (1, 3), (1, -3)), ("c", (1, 4),),
)


def kernel(
    static_hbm, imag_hbm, freq, band, pair_hbm, out,
    rowp, colp, kmat, stat, imag, ahead, acc, red1, red2,
    in_sem, sent, row_recv, col_recv, r1_recv, r1_send, r2_recv, r2_send,
):
    ylo, x, core = (lax.axis_index(a) for a in GROW)
    z, yhi = (lax.axis_index(a) for a in GCOL)
    plane = NX * ylo + x
    row = plane * 2 + core
    col = z * 2 + yhi
    half = rowp.shape[1] // 2
    partner = (ylo, x, 1 - core, z, yhi)
    xs = [lax.rem(x + i, NX) for i in range(NX)]
    zs = [lax.rem(z + i, NZ) for i in range(NZ)]
    cores, ylos, yhis = (core, 1 - core), (ylo, 1 - ylo), (yhi, 1 - yhi)
    in_plane = [
        (ylos[a], xs[b], core, z, yhis[c]) for c in (1, 0) for b in (2, 1, 3, 0) for a in (1, 0) if (a, b, c) != (0, 0, 0)
    ]
    along_z = [
        (ylo, x, cores[a], zs[b], yhi) for b in (4, 3, 5, 2, 6, 1, 7, 0) for a in (1, 0) if (a, b) != (0, 0)
    ]

    loads = [
        pltpu.make_async_copy(pair_hbm, colp.at[row], in_sem.at[0]),
        pltpu.make_async_copy(static_hbm, stat, in_sem.at[1]),
        pltpu.make_async_copy(imag_hbm, imag, in_sem.at[2]),
    ]
    for load in loads:
        load.start()

    barrier = pltpu.get_barrier_semaphore()

    def greet(device):
        pl.semaphore_signal(barrier, inc=1, device_id=device, device_id_type=MESH)

    stays = jnp.logical_and(jnp.logical_and(plane == z, z == 4 * core), core == yhi)
    origin = lax.rem(z + 5 * plane + 4 * yhi, NZ)

    @pl.when(jnp.logical_not(stays))
    def _():
        greet((origin // NX, lax.rem(origin, NX), yhi, plane, core))

    across_y = (ylo, x, core, z, yhis[1])
    beside_y = (ylos[1], x, core, z, yhi)
    near = [beside_y, across_y, partner]
    near += [(ylo, x, core, zs[i], yhi) for i in (1, -1)] + [(ylo, xs[i], core, z, yhi) for i in (1, 2, 3)]
    for device in near:
        greet(device)

    loads[0].wait()
    pl.semaphore_wait(barrier, len(near) + 1 - stays.astype(jnp.int32))

    started = []

    def send(src, dst, recv, device):
        copy = pltpu.make_async_remote_copy(
            src_ref=src, dst_ref=dst, send_sem=sent.at[len(started)], recv_sem=recv,
            device_id=device, device_id_type=MESH,
        )
        started.append(copy)
        return copy

    place = (z // NX, lax.rem(z, NX), yhi, lax.rem(plane + 3 * z + 4 * core, NZ), core)

    def piece(panel, slot, part):
        return panel.at[slot, pl.ds(part * half, half)]

    first = [send(piece(colp, row, t), piece(rowp, row, t), row_recv.at[2 * row + t], place) for t in range(2)]

    @pl.when(jnp.logical_not(stays))
    def _():
        for copy in first:
            copy.start()

    @pl.when(stays)
    def _():
        for t in range(2):
            pltpu.make_async_copy(pair_hbm.at[pl.ds(t * half, half)], piece(rowp, row, t), row_recv.at[2 * row + t]).start()

    starts = {
        (chain, far): 2 * lax.rem(z + 5 * plane + 4 * yhis[chain] + NZ - far, NZ) + yhis[chain]
        for chain in range(2) for far in EVERY
    }

    def block(chain, far):
        return starts[chain, 4 if far == -4 else far]

    arrived = set()

    def need(chain, far, part):
        far = 4 if far == -4 else far
        if (chain, far, part) not in arrived:
            arrived.add((chain, far, part))
            b = block(chain, far)
            pltpu.make_async_copy(piece(rowp, b, part), piece(rowp, b, part), row_recv.at[2 * b + part]).wait()

    def pass_on(chain, far, part, device):
        need(chain, far, part)
        b = block(chain, far)
        send(piece(rowp, b, part), piece(rowp, b, part), row_recv.at[2 * b + part], device).start()

    def along(chain, far, part):
        for way in (1, -1) if far < 3 else ((1,) if part == 0 else (-1,)):
            pass_on(chain, way * far, part, (ylo, x, core, zs[way % NZ], yhi))

    def across(far, part):
        pass_on(0, far, part, across_y)

    def col_slot(a, b, c):
        return 2 * (NX * a + b) + c

    def col_wait(slot):
        pltpu.make_async_copy(colp.at[slot], colp.at[slot], col_recv.at[slot]).wait()

    def col_send(slot, device):
        send(colp.at[slot], colp.at[slot], col_recv.at[slot], device).start()

    def relay(i):
        slot = col_slot(ylos[i // 3], xs[(3, 1, 2)[i % 3]], core)
        col_wait(slot)
        col_send(slot, partner)

    def project(blocks, e):
        left = jnp.concatenate([rowp[b] for b in blocks], axis=0)
        return jnp.dot(left, kmat[e], preferred_element_type=jnp.float32)

    def weighted(projected, b, e):
        terms = projected * colp[b].astype(jnp.float32)
        lanes = terms[:, 0:128]
        for g in range(1, terms.shape[1] // 128):
            lanes = lanes + terms[:, g * 128:(g + 1) * 128]
        total = 0.0
        for part in range(2):
            offset = freq[e] - band[2 * b + part]
            weight = 1.0 / (1.0 + jnp.full((1, 128), offset * offset, jnp.float32))
            total = total + weight * lanes[part * half:(part + 1) * half, :]
        return total

    kept = {}
    places = [(e // 2, slice(e % 2 * half, (e % 2 + 1) * half)) for e in range(NE)]

    def rows_of(n):
        return slice(n * rowp.shape[1], (n + 1) * rowp.shape[1])

    def project_ahead(keys):
        blocks = [block(*key) for key in keys]
        for e in range(NE):
            projected = project(blocks, e)
            for n, key in enumerate(keys):
                ahead[kept.setdefault(key, len(kept)), e] = projected[rows_of(n)]

    def finish(keys):
        for e in range(NE):
            total = acc[places[e]]
            for key in keys:
                total = total + weighted(ahead[kept[key], e], block(*key), e)
            acc[places[e]] = total

    def compute(keys):
        blocks = [block(*key) for key in keys]
        for e in range(NE):
            projected = project(blocks, e)
            total = acc[places[e]]
            for n, b in enumerate(blocks):
                total = total + weighted(projected[rows_of(n)], b, e)
            acc[places[e]] = total

    col_send(row, beside_y)
    col_send(row, partner)
    for dx in (1, 3, 2):
        col_send(row, (ylo, xs[dx], core, z, yhi))

    loads[1].wait()
    loads[2].wait()
    diagonal = row * stat.shape[0] - col * stat.shape[1]
    acc[...] = jnp.zeros_like(acc)

    @pl.loop(0, stat.shape[0] // SLICE)
    def _(i):
        start = pl.multiple_of(i * SLICE, SLICE)
        rows = pl.ds(start, SLICE)
        shape = (SLICE, stat.shape[1])
        ahead = lax.broadcasted_iota(jnp.int32, shape, 1) - lax.broadcasted_iota(jnp.int32, shape, 0)
        one = jnp.where(ahead == diagonal + start, 1.0, 0.0).astype(jnp.float32)
        s = stat[rows, :] - one
        g = imag[rows, :] - one
        d = s - g
        pole = jnp.sqrt((g * g + 0.25) / (d * d + 0.25))
        top = -s * pole
        for e in range(NE):
            kmat[e, rows, :] = (top / (pole + freq[e])).astype(jnp.bfloat16)

    for op, *args in PROGRAM:
        if op == "z":
            along(*args)
        elif op == "y":
            across(*args)
        elif op == "n":
            neighbour = col_slot(ylos[1], x, core)
            col_wait(neighbour)
            for dx in (1, 3, 2):
                col_send(neighbour, (ylo, xs[dx], core, z, yhi))
            col_send(neighbour, partner)
        elif op == "r":
            relay(*args)
        elif op == "w":
            for a in range(2):
                for b in range(NX):
                    col_wait(col_slot(a, b, 1 - core))
        else:
            for chain, far in args:
                need(chain, far, 0)
                need(chain, far, 1)
            {"d": project_ahead, "m": finish, "c": compute}[op](args)

    ones = jnp.ones((8, 128), jnp.float32)
    tile = jnp.concatenate([
        lax.dot_general(
            ones, acc[i], (((1,), (1,)), ((), ())),
            precision=lax.Precision.HIGHEST, preferred_element_type=jnp.float32,
        )[0:1]
        for i in range(2)
    ])

    def exchange(buffer, me, value, devices, recv, sem):
        buffer[me] = value
        copies = [
            pltpu.make_async_remote_copy(
                src_ref=buffer.at[me], dst_ref=buffer.at[me], send_sem=sem.at[i], recv_sem=recv.at[0],
                device_id=device, device_id_type=MESH,
            )
            for i, device in enumerate(devices)
        ]
        for copy in copies:
            copy.start()
        others = buffer.at[pl.ds(0, len(devices))]
        pltpu.make_async_copy(others, others, recv.at[0]).wait()
        total = buffer[0]
        for i in range(1, 16):
            total = total + buffer[i]
        return total, copies

    tile, last = exchange(red2, 2 * z + core, tile, along_z, r2_recv, r2_send)
    out[...], more = exchange(red1, NX * (2 * yhi + ylo) + x, tile, in_plane, r1_recv, r1_send)

    @pl.when(jnp.logical_not(stays))
    def _():
        for copy in first:
            copy.wait_send()

    for copy in started[2:] + last + more:
        copy.wait_send()


def shards(eps_static, eps_imag, frequency_grid, band_energy, pair_elements):
    height, breadth = eps_static.shape
    rows = pair_elements.shape[0] * pair_elements.shape[1]
    pair = pair_elements.reshape(rows, breadth)
    anywhere = pl.BlockSpec(memory_space=pl.ANY)
    scalars = pl.BlockSpec(memory_space=pltpu.SMEM)
    dma = pltpu.SemaphoreType.DMA
    summed = pl.pallas_call(
        kernel,
        out_shape=jax.ShapeDtypeStruct((2, 128), jnp.float32),
        in_specs=[anywhere, anywhere, scalars, scalars, anywhere],
        out_specs=pl.BlockSpec(memory_space=pltpu.VMEM),
        scratch_shapes=[
            pltpu.VMEM((16, rows, height), jnp.bfloat16),
            pltpu.VMEM((16, rows, breadth), jnp.bfloat16),
            pltpu.VMEM((NE, height, breadth), jnp.bfloat16),
            pltpu.VMEM((height, breadth), jnp.float32),
            pltpu.VMEM((height, breadth), jnp.float32),
            pltpu.VMEM((6, NE, rows, breadth), jnp.float32),
            pltpu.VMEM((2, 128, 128), jnp.float32),
            pltpu.VMEM((16, 2, 128), jnp.float32),
            pltpu.VMEM((16, 2, 128), jnp.float32),
            dma((3,)), dma((80,)), dma((32,)), dma((16,)),
            dma((1,)), dma((15,)), dma((1,)), dma((15,)),
        ],
        compiler_params=pltpu.CompilerParams(
            collective_id=0, has_side_effects=True, vmem_limit_bytes=60 * 1024 * 1024
        ),
    )(eps_static, eps_imag, frequency_grid, band_energy, pair)
    states = pair_elements.shape[1] // lax.axis_size(GCOL)
    return lax.dynamic_slice(summed.reshape(4, 64), (0, lax.axis_index(GCOL) * states), (NE, states))


def solution(mesh):
    finer = Mesh(
        mesh.devices.reshape(2, 4, 2, 8, 2), ("grow_0", "grow_1", "grow_2", "gcol_0", "gcol_1")
    )
    in_specs = (P(GROW, GCOL), P(GROW, GCOL), P(), P(), P(GROW, None, GCOL))
    out_specs = P(None, GCOL)
    return jax.shard_map(
        shards, mesh=finer, in_specs=in_specs, out_specs=out_specs, check_vma=False
    )
```

```python
import jax
import jax.numpy as jnp
from jax import lax
from jax.experimental import pallas as pl
from jax.experimental.pallas import tpu as pltpu
from jax.sharding import Mesh
from jax.sharding import PartitionSpec as P

NE = 3
NX = 4
NZ = 8
GROW = ("grow_0", "grow_1", "grow_2")
GCOL = ("gcol_0", "gcol_1")
MESH = pl.DeviceIdType.MESH
SLICE = 16
EVERY = (0, 1, -1, 2, -2, 3, -3, 4)
PARTS = 4
PROGRAM = (
    ("n",),
    ("z", 0, 0, 0),
    ("y", 0, 0),
    ("z", 0, 0, 1),
    ("y", 0, 1),
    ("z", 0, 1, 0),
    ("y", 1, 0),
    ("y", -1, 0),
    ("z", 0, 0, 2),
    ("z", 0, 1, 1),
    ("y", 1, 1),
    ("r", 0),
    ("r", 1),
    ("y", -1, 1),
    ("z", 0, 0, 3),
    ("z", 0, 2, 0),
    ("y", 0, 2),
    ("z", 0, 1, 2),
    ("y", 1, 2),
    ("r", 2),
    ("z", 0, 2, 1),
    ("y", 2, 1),
    ("y", -2, 1),
    ("z", 0, 1, 3),
    ("d", (0, 1), (0, -1)),
    ("r", 3),
    ("y", 3, 0),
    ("z", 1, 1, 0),
    ("y", -3, 0),
    ("z", 0, 2, 2),
    ("y", -1, 2),
    ("z", 0, 2, 3),
    ("r", 4),
    ("y", 0, 3),
    ("z", 1, 2, 1),
    ("d", (0, 2), (0, -2)),
    ("y", 1, 3),
    ("r", 5),
    ("z", 0, 3, 0),
    ("z", 0, 3, 2),
    ("y", -1, 3),
    ("z", 0, 3, 1),
    ("z", 0, 3, 3),
    ("w",),
    ("y", 3, 3),
    ("z", 1, 1, 2),
    ("c", (0, 3), (0, -3)),
    ("y", -3, 3),
    ("z", 1, 3, 1),
    ("y", 4, 0),
    ("c", (0, 0), (1, 0)),
    ("y", 4, 2),
    ("z", 1, 1, 3),
    ("c", (0, 4)),
    ("y", 4, 3),
    ("z", 1, 2, 2),
    ("m", (0, 1), (0, -1), (0, 2), (0, -2)),
    ("c", (1, 1), (1, -1)),
    ("c", (1, 2), (1, -2)),
    ("c", (1, 3), (1, -3)),
    ("c", (1, 4)),
)


def kernel(
    static_hbm, imag_hbm, freq, band, pair_hbm, out,
    rowp, colp, kmat, stat, imag, ahead, acc, red1, red2,
    in_sem, sent, row_recv, col_recv, r1_recv, r1_send, r2_recv, r2_send,
):
    ylo, x, core = (lax.axis_index(a) for a in GROW)
    z, yhi = (lax.axis_index(a) for a in GCOL)
    plane = NX * ylo + x
    row = plane * 2 + core
    col = z * 2 + yhi
    half = rowp.shape[1] // 2
    share = rowp.shape[1] // PARTS
    partner = (ylo, x, 1 - core, z, yhi)
    xs = [lax.rem(x + i, NX) for i in range(NX)]
    zs = [lax.rem(z + i, NZ) for i in range(NZ)]
    cores, ylos, yhis = (core, 1 - core), (ylo, 1 - ylo), (yhi, 1 - yhi)
    in_plane = [
        (ylos[a], xs[b], core, z, yhis[c]) for c in (1, 0) for b in (2, 1, 3, 0) for a in (1, 0) if (a, b, c) != (0, 0, 0)
    ]
    along_z = [
        (ylo, x, cores[a], zs[b], yhi) for b in (4, 3, 5, 2, 6, 1, 7, 0) for a in (1, 0) if (a, b) != (0, 0)
    ]

    loads = [
        pltpu.make_async_copy(pair_hbm, colp.at[row], in_sem.at[0]),
        pltpu.make_async_copy(static_hbm, stat, in_sem.at[1]),
        pltpu.make_async_copy(imag_hbm, imag, in_sem.at[2]),
    ]
    for load in loads:
        load.start()

    barrier = pltpu.get_barrier_semaphore()

    def greet(device):
        pl.semaphore_signal(barrier, inc=1, device_id=device, device_id_type=MESH)

    stays = jnp.logical_and(jnp.logical_and(plane == z, z == 4 * core), core == yhi)
    origin = lax.rem(z + 5 * plane + 4 * yhi, NZ)

    @pl.when(jnp.logical_not(stays))
    def _():
        greet((origin // NX, lax.rem(origin, NX), yhi, plane, core))

    across_y = (ylo, x, core, z, yhis[1])
    beside_y = (ylos[1], x, core, z, yhi)
    near = [beside_y, across_y, partner]
    near += [(ylo, x, core, zs[i], yhi) for i in (1, -1)] + [(ylo, xs[i], core, z, yhi) for i in (1, 2, 3)]
    for device in near:
        greet(device)

    loads[0].wait()
    pl.semaphore_wait(barrier, len(near) + 1 - stays.astype(jnp.int32))

    started = []

    def send(src, dst, recv, device):
        copy = pltpu.make_async_remote_copy(
            src_ref=src, dst_ref=dst, send_sem=sent.at[len(started)], recv_sem=recv,
            device_id=device, device_id_type=MESH,
        )
        started.append(copy)
        return copy

    place = (z // NX, lax.rem(z, NX), yhi, lax.rem(plane + 3 * z + 4 * core, NZ), core)

    def piece(panel, slot, part):
        return panel.at[slot, pl.ds(part * share, share)]

    first = [send(piece(colp, row, t), piece(rowp, row, t), row_recv.at[PARTS * row + t], place) for t in range(PARTS)]

    @pl.when(jnp.logical_not(stays))
    def _():
        for copy in first:
            copy.start()

    @pl.when(stays)
    def _():
        for t in range(PARTS):
            pltpu.make_async_copy(pair_hbm.at[pl.ds(t * share, share)], piece(rowp, row, t), row_recv.at[PARTS * row + t]).start()

    starts = {
        (chain, far): 2 * lax.rem(z + 5 * plane + 4 * yhis[chain] + NZ - far, NZ) + yhis[chain]
        for chain in range(2) for far in EVERY
    }

    def block(chain, far):
        return starts[chain, 4 if far == -4 else far]

    arrived = set()

    def need(chain, far, part):
        far = 4 if far == -4 else far
        if (chain, far, part) not in arrived:
            arrived.add((chain, far, part))
            b = block(chain, far)
            pltpu.make_async_copy(piece(rowp, b, part), piece(rowp, b, part), row_recv.at[PARTS * b + part]).wait()

    def pass_on(chain, far, part, device):
        need(chain, far, part)
        b = block(chain, far)
        send(piece(rowp, b, part), piece(rowp, b, part), row_recv.at[PARTS * b + part], device).start()

    def along(chain, far, part):
        for way in (1, -1) if far < 3 else ((1,) if part < PARTS // 2 else (-1,)):
            pass_on(chain, way * far, part, (ylo, x, core, zs[way % NZ], yhi))

    def across(far, part):
        pass_on(0, far, part, across_y)

    def col_slot(a, b, c):
        return 2 * (NX * a + b) + c

    def col_wait(slot):
        pltpu.make_async_copy(colp.at[slot], colp.at[slot], col_recv.at[slot]).wait()

    def col_send(slot, device):
        send(colp.at[slot], colp.at[slot], col_recv.at[slot], device).start()

    def relay(i):
        slot = col_slot(ylos[i // 3], xs[(3, 1, 2)[i % 3]], core)
        col_wait(slot)
        col_send(slot, partner)

    def project(blocks, e):
        left = jnp.concatenate([rowp[b] for b in blocks], axis=0)
        return jnp.dot(left, kmat[e], preferred_element_type=jnp.float32)

    def weighted(projected, b, e):
        terms = projected * colp[b].astype(jnp.float32)
        lanes = terms[:, 0:128]
        for g in range(1, terms.shape[1] // 128):
            lanes = lanes + terms[:, g * 128:(g + 1) * 128]
        total = 0.0
        for part in range(2):
            offset = freq[e] - band[2 * b + part]
            weight = 1.0 / (1.0 + jnp.full((1, 128), offset * offset, jnp.float32))
            total = total + weight * lanes[part * half:(part + 1) * half, :]
        return total

    kept = {}
    places = [(e // 2, slice(e % 2 * half, (e % 2 + 1) * half)) for e in range(NE)]

    def rows_of(n):
        return slice(n * rowp.shape[1], (n + 1) * rowp.shape[1])

    def project_ahead(keys):
        blocks = [block(*key) for key in keys]
        for e in range(NE):
            projected = project(blocks, e)
            for n, key in enumerate(keys):
                ahead[kept.setdefault(key, len(kept)), e] = projected[rows_of(n)]

    def finish(keys):
        for e in range(NE):
            total = acc[places[e]]
            for key in keys:
                total = total + weighted(ahead[kept[key], e], block(*key), e)
            acc[places[e]] = total

    def compute(keys):
        blocks = [block(*key) for key in keys]
        for e in range(NE):
            projected = project(blocks, e)
            total = acc[places[e]]
            for n, b in enumerate(blocks):
                total = total + weighted(projected[rows_of(n)], b, e)
            acc[places[e]] = total

    col_send(row, beside_y)
    col_send(row, partner)
    for dx in (1, 3, 2):
        col_send(row, (ylo, xs[dx], core, z, yhi))

    loads[1].wait()
    loads[2].wait()
    diagonal = row * stat.shape[0] - col * stat.shape[1]
    acc[...] = jnp.zeros_like(acc)

    @pl.loop(0, stat.shape[0] // SLICE)
    def _(i):
        start = pl.multiple_of(i * SLICE, SLICE)
        rows = pl.ds(start, SLICE)
        shape = (SLICE, stat.shape[1])
        ahead = lax.broadcasted_iota(jnp.int32, shape, 1) - lax.broadcasted_iota(jnp.int32, shape, 0)
        one = jnp.where(ahead == diagonal + start, 1.0, 0.0).astype(jnp.float32)
        s = stat[rows, :] - one
        g = imag[rows, :] - one
        d = s - g
        pole = jnp.sqrt((g * g + 0.25) / (d * d + 0.25))
        top = -s * pole
        for e in range(NE):
            kmat[e, rows, :] = (top / (pole + freq[e])).astype(jnp.bfloat16)

    for op, *args in PROGRAM:
        if op == "z":
            along(*args)
        elif op == "y":
            across(*args)
        elif op == "n":
            neighbour = col_slot(ylos[1], x, core)
            col_wait(neighbour)
            for dx in (1, 3, 2):
                col_send(neighbour, (ylo, xs[dx], core, z, yhi))
            col_send(neighbour, partner)
        elif op == "r":
            relay(*args)
        elif op == "w":
            for a in range(2):
                for b in range(NX):
                    col_wait(col_slot(a, b, 1 - core))
        else:
            for chain, far in args:
                for part in range(PARTS):
                    need(chain, far, part)
            {"d": project_ahead, "m": finish, "c": compute}[op](args)

    ones = jnp.ones((8, 128), jnp.float32)
    tile = jnp.concatenate([
        lax.dot_general(
            ones, acc[i], (((1,), (1,)), ((), ())),
            precision=lax.Precision.HIGHEST, preferred_element_type=jnp.float32,
        )[0:1]
        for i in range(2)
    ])

    def exchange(buffer, me, value, devices, recv, sem):
        buffer[me] = value
        copies = [
            pltpu.make_async_remote_copy(
                src_ref=buffer.at[me], dst_ref=buffer.at[me], send_sem=sem.at[i], recv_sem=recv.at[0],
                device_id=device, device_id_type=MESH,
            )
            for i, device in enumerate(devices)
        ]
        for copy in copies:
            copy.start()
        others = buffer.at[pl.ds(0, len(devices))]
        pltpu.make_async_copy(others, others, recv.at[0]).wait()
        total = buffer[0]
        for i in range(1, 16):
            total = total + buffer[i]
        return total, copies

    tile, last = exchange(red2, 2 * z + core, tile, along_z, r2_recv, r2_send)
    out[...], more = exchange(red1, NX * (2 * yhi + ylo) + x, tile, in_plane, r1_recv, r1_send)

    @pl.when(jnp.logical_not(stays))
    def _():
        for copy in first:
            copy.wait_send()

    for copy in started[PARTS:] + last + more:
        copy.wait_send()


def shards(eps_static, eps_imag, frequency_grid, band_energy, pair_elements):
    height, breadth = eps_static.shape
    rows = pair_elements.shape[0] * pair_elements.shape[1]
    pair = pair_elements.reshape(rows, breadth)
    anywhere = pl.BlockSpec(memory_space=pl.ANY)
    scalars = pl.BlockSpec(memory_space=pltpu.SMEM)
    dma = pltpu.SemaphoreType.DMA
    summed = pl.pallas_call(
        kernel,
        out_shape=jax.ShapeDtypeStruct((2, 128), jnp.float32),
        in_specs=[anywhere, anywhere, scalars, scalars, anywhere],
        out_specs=pl.BlockSpec(memory_space=pltpu.VMEM),
        scratch_shapes=[
            pltpu.VMEM((16, rows, height), jnp.bfloat16),
            pltpu.VMEM((16, rows, breadth), jnp.bfloat16),
            pltpu.VMEM((NE, height, breadth), jnp.bfloat16),
            pltpu.VMEM((height, breadth), jnp.float32),
            pltpu.VMEM((height, breadth), jnp.float32),
            pltpu.VMEM((4, NE, rows, breadth), jnp.float32),
            pltpu.VMEM((2, 128, 128), jnp.float32),
            pltpu.VMEM((16, 2, 128), jnp.float32),
            pltpu.VMEM((16, 2, 128), jnp.float32),
            dma((3,)), dma((128,)), dma((16 * PARTS,)), dma((16,)),
            dma((1,)), dma((15,)), dma((1,)), dma((15,)),
        ],
        compiler_params=pltpu.CompilerParams(
            collective_id=0, has_side_effects=True, vmem_limit_bytes=60 * 1024 * 1024
        ),
    )(eps_static, eps_imag, frequency_grid, band_energy, pair)
    states = pair_elements.shape[1] // lax.axis_size(GCOL)
    return lax.dynamic_slice(summed.reshape(4, 64), (0, lax.axis_index(GCOL) * states), (NE, states))


def solution(mesh):
    finer = Mesh(
        mesh.devices.reshape(2, 4, 2, 8, 2), ("grow_0", "grow_1", "grow_2", "gcol_0", "gcol_1")
    )
    in_specs = (P(GROW, GCOL), P(GROW, GCOL), P(), P(), P(GROW, None, GCOL))
    out_specs = P(None, GCOL)
    return jax.shard_map(
        shards, mesh=finer, in_specs=in_specs, out_specs=out_specs, check_vma=False
    )
```
